32 devices in a mesh: au: 4 (over y, x), pa: 4 (over z), dev: 2 (over core).
Axes of the slice: x: 2, y: 2, z: 4, core: 2. Of those that a mesh axis runs over, the one named last changes fastest.
Arguments:
- features: bfloat16 [4096, 64, 256], P('au', 'pa'), may hold values from -6 to 6
- item_ids: int32 [4096, 64], P('au', 'pa'), may hold values from 0 to 4095
- item_table: bfloat16 [4096, 256], replicated, may hold values from -4 to 4
- lengths: int32 [4096], P('au'), may hold values from 1 to 64
- routing_seed: int32 [4, 64], replicated, may hold values from 0 to 15
- w_qkv: bfloat16 [3, 256, 256], P(None, None, 'dev'), may hold values from -0.375 to 0.375
- w_out: bfloat16 [256, 256], P('dev'), may hold values from -0.375 to 0.375
- w_bilinear: bfloat16 [256, 256], P(None, 'dev'), may hold values from -0.375 to 0.375
- w_up: bfloat16 [256, 1024], P(None, 'dev'), may hold values from -0.375 to 0.375
- w_down: bfloat16 [1024, 256], P('dev'), may hold values from -0.1875 to 0.1875
Outputs:
- capsules: float32 [4096, 4, 256], P(('au', 'pa'), None, 'dev')
The draws below stay inside these ranges and needn't reach their ends.
All inputs are finite; a program needn't handle non-finite values.
Results may differ from the reference program's by a relative error of at most 0.012.
The reference program's roundings to bfloat16 on the way (of `inputs`, `rounded`, `attended`, `hidden` and `interest`) count: a program that leaves them out, or rounds other values in their place, can miss the bound.
Values may be sent and summed in bfloat16 or wider, within the bound.
A program may use at most 128 MiB of HBM per device.

```python
import math
import jax
import jax.numpy as jnp
import numpy as np
from jax import lax

D = 256
HEADS = 4
FF = 1024
CATS = 4096
HISTORY = 64
CAPS = 4
ITERS = 3
USERS_DEV = 1024
USERS = 4096


def set_ends(entries, rng, least, top_value):
    longest = entries.shape.index(max(entries.shape))
    spots = []
    for shift in (0, 1):
        where = [jax.random.randint(jax.random.fold_in(rng, axis), (), 0, length) for axis, length in enumerate(entries.shape)]
        where[longest] = (where[longest] + shift) % entries.shape[longest]
        spots.append(tuple(where))
    return entries.at[spots[0]].set(least).at[spots[1]].set(top_value)


def block_scale(stream_key, shape, shards, smallest, top_value):
    def one(dim, shards_of):
        heights = jax.random.uniform(jax.random.fold_in(jax.random.fold_in(stream_key, 6), dim), (shards_of,), jnp.float32, smallest / len(shards), top_value / len(shards))
        return jnp.repeat(jnp.exp(heights), shape[dim] // shards_of).reshape((-1,) + (1,) * (len(shape) - dim - 1))

    level = one(*shards[0])
    for cut in shards[1:]:
        level = level * one(*cut)
    return level


def rank_bounds(number_of, lean):
    portions = [(1 << 20) // math.isqrt(grade ** lean) + 1 for grade in range(1, number_of + 1)]
    width = 1 + sum(portions) // (1 << 30)
    return np.cumsum(np.array([max(1, weight // width) for weight in portions]))


def ranked_ids(key, extent, count, lean):
    grid = rank_bounds(count, lean)
    lot = jax.random.randint(jax.random.fold_in(key, 1), extent, 0, int(grid[count - 1]))
    standing = jnp.searchsorted(jnp.asarray(grid, jnp.int32), lot, side="right")
    return jax.random.permutation(jax.random.fold_in(key, 2), count)[standing].astype(jnp.int32)


def bell_draw(key, extent, spread, bound, split=(), kind=jnp.bfloat16):
    gain = block_scale(key, extent, split, -0.22, 0.18) if split else 1.0
    values = jax.random.normal(key, extent, jnp.float32) * spread * gain
    return jnp.minimum(jnp.maximum(values, -bound), bound).astype(kind)


def setup_inputs(seed: int = 0) -> dict:
    keys = jax.random.split(jax.random.key(seed), 11)
    return {
        "features": bell_draw(keys[0], (USERS, HISTORY, D), 1.0, 6.0, ((0, 4), (1, 4))),
        "item_ids": set_ends(ranked_ids(keys[1], (USERS, HISTORY), CATS, 2), jax.random.fold_in(keys[1], 3), 0, CATS - 1).astype(jnp.int32),
        "item_table": bell_draw(keys[2], (CATS, D), 0.7, 4.0),
        "lengths": set_ends(jax.random.randint(keys[3], (USERS,), 1, HISTORY + 1), jax.random.fold_in(keys[3], 1), 1, HISTORY).astype(jnp.int32),
        "routing_seed": set_ends(jax.random.randint(keys[4], (CAPS, HISTORY), 0, 16), jax.random.fold_in(keys[4], 1), 0, 15).astype(jnp.int32),
        "w_qkv": bell_draw(keys[5], (3, D, D), D ** -0.5, 0.375, ((2, 2),)),
        "w_out": bell_draw(keys[6], (D, D), D ** -0.5, 0.375, ((0, 2),)),
        "w_bilinear": bell_draw(keys[7], (D, D), D ** -0.5, 0.375, ((1, 2),)),
        "w_up": bell_draw(keys[8], (D, FF), D ** -0.5, 0.375, ((1, 2),)),
        "w_down": bell_draw(keys[9], (FF, D), FF ** -0.5, 0.1875, ((0, 2),)),
    }


def widen(array):
    return lax.optimization_barrier(array).astype(jnp.float32)

def route(interest, valid, routing_seed):
    vectors = widen(interest)
    user_count = vectors.shape[0]
    base = (routing_seed.astype(jnp.float32) - 7.5) * 0.25
    logits = jnp.broadcast_to(base[None], (user_count, CAPS, HISTORY))
    capsules = jnp.zeros((user_count, CAPS, vectors.shape[2]), jnp.float32)
    for sweep in range(ITERS):
        weights = jax.nn.softmax(logits, axis=1) * valid[:, None, :]
        summed = jnp.einsum('ukl,uld->ukd', weights, vectors, precision=lax.Precision.HIGHEST)
        squares = lax.optimization_barrier(jnp.sum(summed * summed, axis=-1))
        factor = jnp.sqrt(squares) / (1.0 + squares)
        capsules = summed * factor[..., None]
        if sweep + 1 < ITERS:
            logits = logits + jnp.einsum('ukd,uld->ukl', capsules, vectors, precision=lax.Precision.HIGHEST)
    return capsules

def encode(feats, ids, user_lengths, item_table, routing_seed, w_qkv, w_out, w_bilinear, w_up, w_down):
    user_count = feats.shape[0]
    head_size = D // HEADS
    inputs = (feats.astype(jnp.float32) + item_table[ids].astype(jnp.float32)).astype(jnp.bfloat16)
    flat_rows = inputs.reshape(-1, D)

    def project(index):
        made = jnp.dot(flat_rows, w_qkv[index], preferred_element_type=jnp.float32).astype(jnp.bfloat16)
        return widen(made.reshape(user_count, HISTORY, HEADS, head_size))
    queries = project(0)
    key_block = project(1)
    value_block = project(2)
    scores = jnp.einsum('uqhe,ukhe->uqhk', queries, key_block, precision=lax.Precision.HIGHEST) * (1.0 / head_size ** 0.5)
    valid_keys = jnp.arange(HISTORY)[None, :] < user_lengths[:, None]
    mask_four = valid_keys[:, None, None, :]
    probs = jnp.where(mask_four, jnp.exp(scores), 0.0)
    totals = lax.optimization_barrier(jnp.sum(probs, axis=-1))
    rounded = widen(probs.astype(jnp.bfloat16))
    weighted = jnp.einsum('uqhk,ukhe->uqhe', rounded, value_block, precision=lax.Precision.HIGHEST)
    attended = (weighted / totals[..., None]).astype(jnp.bfloat16).reshape(-1, D)
    hidden = jax.nn.gelu(jnp.dot(flat_rows, w_up, preferred_element_type=jnp.float32)).astype(jnp.bfloat16)
    interest = (jnp.dot(flat_rows, w_bilinear, preferred_element_type=jnp.float32) + jnp.dot(attended, w_out, preferred_element_type=jnp.float32) + jnp.dot(hidden, w_down, preferred_element_type=jnp.float32)).astype(jnp.bfloat16)
    interest = interest.reshape(user_count, HISTORY, D)
    return route(interest, valid_keys.astype(jnp.float32), routing_seed)

def reference(features, item_ids, item_table, lengths, routing_seed, w_qkv, w_out, w_bilinear, w_up, w_down):
    blocks = USERS // USERS_DEV
    feat_blocks = features.reshape(blocks, USERS_DEV, HISTORY, D)
    id_blocks = item_ids.reshape(blocks, USERS_DEV, HISTORY)
    length_blocks = lengths.reshape(blocks, USERS_DEV)

    def one_block(group):
        return encode(group[0], group[1], group[2], item_table, routing_seed, w_qkv, w_out, w_bilinear, w_up, w_down)
    result = lax.map(one_block, (feat_blocks, id_blocks, length_blocks))
    return result.reshape(USERS, CAPS, D)
```

```python
import functools

import jax
import jax.numpy as jnp
from jax import lax
from jax.experimental import pallas as pl
from jax.experimental.pallas import tpu as pltpu
from jax.sharding import PartitionSpec as P

D = 256
HEADS = 4
CAPS = 4
ITERS = 3


def local_routing(vectors, valid, base):
    user_count, history_len, width_here = vectors.shape
    logits = jnp.broadcast_to(base[None], (user_count, CAPS, history_len))
    capsules = jnp.zeros((user_count, CAPS, width_here), jnp.float32)
    for sweep in range(ITERS):
        weights = jax.nn.softmax(logits, axis=1) * valid[:, None, :]
        summed = jnp.einsum("ukl,uld->ukd", weights, vectors, precision=lax.Precision.HIGHEST)
        squares = jnp.sum(summed * summed, axis=-1)
        factor = jnp.sqrt(squares) / (1.0 + squares)
        capsules = summed * factor[..., None]
        if sweep + 1 < ITERS:
            logits = logits + jnp.einsum(
                "ukd,uld->ukl", capsules, vectors, precision=lax.Precision.HIGHEST
            )
    return capsules


def plain_body(
    features, item_ids, item_table, lengths, routing_seed, w_qkv, w_out, w_bilinear, w_up, w_down
):
    pa_count = lax.axis_size("pa")
    dev_count = lax.axis_size("dev")
    owned_users = lengths.shape[0] // pa_count
    head_size = D // HEADS
    share = owned_users // dev_count
    core = lax.axis_index("dev")

    def pick(array):
        shaped = array.reshape((pa_count, dev_count, share) + array.shape[1:])
        chosen = lax.dynamic_index_in_dim(shaped, core, 1, keepdims=False)
        return chosen.reshape((pa_count * share,) + array.shape[1:])

    features = pick(features)
    item_ids = pick(item_ids)
    lengths = pick(lengths)
    w_qkv, w_out, w_bilinear, w_up, w_down = (
        lax.all_gather(w_qkv, "dev", axis=2, tiled=True),
        lax.all_gather(w_out, "dev", axis=0, tiled=True),
        lax.all_gather(w_bilinear, "dev", axis=1, tiled=True),
        lax.all_gather(w_up, "dev", axis=1, tiled=True),
        lax.all_gather(w_down, "dev", axis=0, tiled=True),
    )
    own_lens = lax.dynamic_slice_in_dim(lengths, lax.axis_index("pa") * share, share)
    features, item_ids = (
        lax.all_to_all(features, "pa", split_axis=0, concat_axis=1, tiled=True),
        lax.all_to_all(item_ids, "pa", split_axis=0, concat_axis=1, tiled=True),
    )
    user_count, span_here, model_width = features.shape
    heads_here = w_qkv.shape[2] // head_size
    inputs = (
        features.astype(jnp.float32) + jnp.take(item_table, item_ids, axis=0).astype(jnp.float32)
    ).astype(jnp.bfloat16)
    flat_rows = inputs.reshape(-1, model_width)

    def project(index):
        shaped = w_qkv[index].reshape(model_width, heads_here, head_size)
        made = jnp.einsum(
            "nd,dhe->hne", flat_rows, shaped, preferred_element_type=jnp.float32
        ).astype(jnp.bfloat16)
        return made.reshape(heads_here, user_count, span_here, head_size)

    queries = project(0)
    key_block = project(1)
    value_block = project(2)
    score_scale = 1.0 / head_size**0.5
    count_here = key_block.shape[2]
    scores = (
        jnp.einsum("huqe,huke->huqk", queries, key_block, preferred_element_type=jnp.float32)
        * score_scale
    )
    positions = jnp.arange(count_here, dtype=jnp.int32)
    valid_keys = positions[None, :] < own_lens[:, None]
    mask_four = valid_keys[None, :, None, :]
    probs = jnp.where(mask_four, jnp.exp(scores), 0.0)
    totals = jnp.sum(probs, axis=-1)
    weighted = jnp.einsum(
        "huqk,huke->huqe",
        probs.astype(jnp.bfloat16),
        value_block,
        preferred_element_type=jnp.float32,
    )
    attended = (weighted / totals[..., None]).astype(jnp.bfloat16)
    out_heads = w_out.reshape(heads_here, head_size, w_out.shape[1])
    attended_term = jnp.einsum(
        "huqe,hef->uqf", attended, out_heads, preferred_element_type=jnp.float32
    )
    hidden = jax.nn.gelu(jnp.dot(flat_rows, w_up, preferred_element_type=jnp.float32)).astype(
        jnp.bfloat16
    )
    partial_terms = attended_term.reshape(-1, w_out.shape[1]) + jnp.dot(
        hidden, w_down, preferred_element_type=jnp.float32
    )
    interest_in = (
        partial_terms + jnp.dot(flat_rows, w_bilinear, preferred_element_type=jnp.float32)
    ).astype(jnp.bfloat16)
    interest_in = interest_in.reshape(user_count, span_here, -1)
    history_len = interest_in.shape[1]
    valid = (jnp.arange(history_len)[None, :] < own_lens[:, None]).astype(jnp.float32)
    base = (routing_seed.astype(jnp.float32) - 7.5) * 0.25
    routed = local_routing(interest_in.astype(jnp.float32), valid, base)
    capsules = lax.all_to_all(routed, "dev", split_axis=2, concat_axis=0, tiled=True)
    return capsules


GROUP = 8
F32, BF16 = jnp.float32, jnp.bfloat16
NT = (((1,), (1,)), ((), ()))
MESH = pl.DeviceIdType.MESH


def dot(a, b):
    return jnp.dot(a, b, preferred_element_type=F32)


def split(a):
    high = a.astype(BF16)
    low = (a - high.astype(F32)).astype(BF16)
    return jnp.concatenate([high, low], axis=0)


def interleave(*parts):
    parts = list(parts)
    while parts:
        for part in list(parts):
            try:
                next(part)
            except StopIteration:
                parts.remove(part)


def fused(
    n, share, ids, lens, feats, table, seed, w_qkv, w_out, w_bil, w_up, w_down,
    out, recv, ids_vmem, ids_smem, table_in, table_wide, rows, x_ref, base, w_in, w_mix, blocks,
    qkv, mix, high, low, weighted, interests, outbox,
    table_sem, own_sem, id_sem, idsend_sem, idrecv_sem, wown_sem, wsend_sem, wrecv_sem,
    send_sem, recv_sem, xsend_sem, xrecv_sem,
):
    me = lax.axis_index("pa")
    core = lax.axis_index("dev")
    sibling = 1 - core
    span, width = feats.shape[1], feats.shape[2]
    history = n * span
    head = width // HEADS
    half = width // 2
    chunks = share // GROUP
    part = GROUP // 2
    pieces = [(c * GROUP, GROUP) for c in range(chunks - 1)]
    pieces += [(share - GROUP, part), (share - part, part)]

    def owner(step):
        return lax.rem(me + step + 1, n)

    def first_user(who):
        return pl.multiple_of((who * 2 + core) * share, share)

    barrier = pltpu.get_barrier_semaphore()
    for step in range(n - 1):
        pl.semaphore_signal(barrier, inc=1, device_id={"pa": owner(step)}, device_id_type=MESH)
    pl.semaphore_signal(barrier, inc=1, device_id={"dev": sibling}, device_id_type=MESH)

    table_copy = pltpu.make_async_copy(table, table_in, table_sem)
    table_copy.start()
    own_feats = pltpu.make_async_copy(
        feats.at[pl.ds(first_user(me), share)],
        recv.at[:, pl.ds(pl.multiple_of(me * span, span), span), :],
        own_sem,
    )
    own_feats.start()
    own_ids = pltpu.make_async_copy(
        ids.at[:, pl.ds(first_user(me), share)], ids_vmem.at[me], id_sem.at[0]
    )
    own_ids.start()

    up_half = w_up.shape[1]
    down_half = w_down.shape[0]

    def cols(start, size):
        return pl.ds(pl.multiple_of(start, 128), size)

    weights = [
        (w_qkv.at[i], w_in.at[:, cols(i * width + core * half, half)]) for i in range(3)
    ] + [
        (w_up, w_in.at[:, cols(3 * width + core * up_half, up_half)]),
        (w_bil, w_mix.at[pl.ds(0, width), cols(core * half, half)]),
        (w_out, w_mix.at[cols(width + core * half, half), :]),
        (w_down, w_mix.at[cols(2 * width + core * down_half, down_half), :]),
    ]
    own_copies = []
    for i, (source, target) in enumerate(weights):
        copy = pltpu.make_async_copy(source, target, wown_sem.at[i])
        copy.start()
        own_copies.append(copy)

    def send_ids(step):
        return pltpu.make_async_remote_copy(
            ids.at[:, pl.ds(first_user(owner(step)), share)],
            ids_vmem.at[me],
            idsend_sem.at[step],
            idrecv_sem.at[step],
            device_id={"pa": owner(step)},
            device_id_type=MESH,
        )

    def send_of(p, start, size, step):
        return pltpu.make_async_remote_copy(
            feats.at[pl.ds(first_user(owner(step)) + start, size)],
            recv.at[pl.ds(start, size), pl.ds(pl.multiple_of(me * span, span), span), :],
            send_sem.at[p, step],
            recv_sem.at[p, step],
            device_id={"pa": owner(step)},
            device_id_type=MESH,
        )

    wcopies = []
    for i, (source, target) in enumerate(weights):
        wcopies.append(
            pltpu.make_async_remote_copy(
                source, target, wsend_sem.at[i], wrecv_sem.at[i],
                device_id={"dev": sibling}, device_id_type=MESH,
            )
        )

    pl.semaphore_wait(barrier, n)
    for step in range(n - 1):
        send_ids(step).start()

    def launch(c, carry):
        for step in range(n - 1):
            send_of(c, c * GROUP, GROUP, step).start()
        return carry

    launch(0, 0)
    for copy in wcopies:
        copy.start()
    lax.fori_loop(1, chunks - 1, launch, 0)
    for p in (chunks - 1, chunks):
        for step in range(n - 1):
            send_of(p, *pieces[p], step).start()

    base_here = (seed[...].astype(F32) - 7.5) * 0.25
    base_here = jnp.concatenate([base_here] * GROUP, axis=1)
    for j in range(CAPS):
        base[j * GROUP : (j + 1) * GROUP, :] = jnp.broadcast_to(
            base_here[j : j + 1], (GROUP, GROUP * history)
        )
    blocks[...] = (
        lax.broadcasted_iota(jnp.int32, blocks.shape, 0) // history
        == lax.broadcasted_iota(jnp.int32, blocks.shape, 1) // head
    ).astype(F32).astype(BF16)

    table_copy.wait()

    def widen(i, carry):
        at = pl.ds(pl.multiple_of(i * 256, 256), 256)
        for h in range(2):
            table_wide[pl.ds(pl.multiple_of(i * 512, 512) + h, 256, stride=2), :] = table_in[
                at, h * half : (h + 1) * half
            ].astype(F32)
        return carry

    lax.fori_loop(0, table_in.shape[0] // 256, widen, 0)

    own_ids.wait()
    for step in range(n - 1):
        send_ids(step).wait_recv()
    id_copy = pltpu.make_async_copy(ids_vmem, ids_smem, id_sem.at[1])
    id_copy.start()
    id_copy.wait()

    def gather(c):
        def fetch(u, carry):
            for z in range(n):
                for p in range(span):
                    spot = pl.multiple_of(u * 2 * history, 2 * history) + 2 * (z * span + p)
                    rows[pl.ds(spot, 2), :] = table_wide[
                        pl.ds(ids_smem[z, p, c * GROUP + u] * 2, 2), :
                    ]
            return carry

        lax.fori_loop(0, GROUP, fetch, 0)

    ff = w_in.shape[1] - 3 * width
    span_rows = GROUP * history
    lane = lax.broadcasted_iota(jnp.int32, (history, HEADS * history), 1)
    key_spot = lax.rem(lane, history)

    def lengths_of(g):
        length_at = (me * 2 + core) * share + g * GROUP
        return [lens[length_at + u] for u in range(GROUP)]

    def encode(g, first=0, users=GROUP):
        lengths = lengths_of(g)
        span_here = slice(first * history, (first + users) * history)
        count = users * history
        feats_here = recv[pl.ds(g * GROUP + first, users)].reshape(count, width)
        for h in range(2):
            columns = slice(h * half, (h + 1) * half)
            x_ref[span_here, columns] = (
                feats_here[:, columns].astype(F32)
                + rows[pl.ds(2 * first * history + h, count, stride=2), :]
            ).astype(BF16)
        x = x_ref[span_here, :]
        for f in range(0, 3 * width, width):
            qkv[span_here, f : f + width] = dot(x, w_in[:, f : f + width]).astype(BF16)
            yield
        ats = [(u, pl.ds(u * history, history)) for u in range(first, first + users)]
        for u, at in ats:
            keys = jnp.concatenate([qkv[at, width : 2 * width]] * HEADS, axis=0) * blocks[...]
            scores = lax.dot_general(
                qkv[at, :width], keys, NT, preferred_element_type=F32
            ) * (1.0 / head**0.5)
            probs = jnp.where(key_spot < lengths[u], jnp.exp(scores), 0.0)
            top = probs.astype(BF16)
            high[at, :] = top
            low[at, :] = (probs - top.astype(F32)).astype(BF16)
            if u % 2:
                yield
        for f in range(0, ff, 256):
            up = dot(x, w_in[:, 3 * width + f : 3 * width + f + 256])
            mix[span_here, width + f : width + f + 256] = jax.nn.gelu(up).astype(BF16)
            yield
        for u, at in ats:
            values = jnp.concatenate([qkv[at, 2 * width :]] * HEADS, axis=0) * blocks[...]
            weighted[at, :] = dot(high[at, :], values)
            if u % 2:
                yield
        totals = dot(high[span_here, :], blocks[...]) + dot(low[span_here, :], blocks[...])
        mix[span_here, :width] = (weighted[span_here, :] / totals).astype(BF16)
        yield
        made = (dot(x, w_mix[:width, :]) + dot(mix[span_here, :], w_mix[width:, :])).astype(BF16)
        interests[lax.rem(g, 2), span_here, :] = made

    def route(g):
        lengths = lengths_of(g)
        slot = lax.rem(g, 2)
        row = lax.broadcasted_iota(jnp.int32, (GROUP, span_rows), 0)
        col = lax.broadcasted_iota(jnp.int32, (GROUP, span_rows), 1)
        limit = jnp.zeros((GROUP, span_rows), jnp.int32)
        for u in range(GROUP):
            limit = jnp.where(row == u, u * history + lengths[u], limit)
        valid = ((col >= row * history) & (col < limit)).astype(F32)
        logits = [base[j * GROUP : (j + 1) * GROUP, :] for j in range(CAPS)]
        capsules = None
        for sweep in range(ITERS):
            peak = functools.reduce(jnp.maximum, logits)
            powers = [jnp.exp(l - peak) for l in logits]
            scale = valid / functools.reduce(jnp.add, powers)
            weights_here = jnp.concatenate([p * scale for p in powers], axis=0)
            both = dot(split(weights_here), interests[slot])
            yield
            yield
            summed = both[: CAPS * GROUP] + both[CAPS * GROUP :]
            squares = jnp.sum(summed * summed, axis=1, keepdims=True)
            yield
            capsules = summed * (jnp.sqrt(squares) / (1.0 + squares))
            if sweep + 1 < ITERS:
                both = lax.dot_general(
                    split(capsules), interests[slot], NT, preferred_element_type=F32
                )
                yield
                yield
                gain = both[: CAPS * GROUP] + both[CAPS * GROUP :]
                logits = [
                    l + gain[j * GROUP : (j + 1) * GROUP] for j, l in enumerate(logits)
                ]
        mine = jnp.where(core == 0, capsules[:, :half], capsules[:, half:])
        theirs = jnp.where(core == 0, capsules[:, half:], capsules[:, :half])
        first = g * GROUP * CAPS
        for j in range(CAPS):
            here = slice(j * GROUP, (j + 1) * GROUP)
            spot = pl.multiple_of(core * share * CAPS + first, GROUP * CAPS) + j
            out[pl.ds(spot, GROUP, stride=CAPS), :] = mine[here]
            spot = pl.multiple_of(first, GROUP * CAPS) + j
            outbox[pl.ds(spot, GROUP, stride=CAPS), :] = theirs[here]

    size = GROUP * CAPS

    def exchange(c):
        return pltpu.make_async_remote_copy(
            outbox.at[pl.ds(pl.multiple_of(c * size, size), size), :],
            out.at[pl.ds(pl.multiple_of(core * share * CAPS + c * size, size), size), :],
            xsend_sem.at[c],
            xrecv_sem.at[c],
            device_id={"dev": sibling},
            device_id_type=MESH,
        )

    def arrive(p, start, size):
        for step in range(n - 1):
            send_of(p, start, size, step).wait_recv()

    gather(0)
    own_feats.wait()
    for copy in own_copies:
        copy.wait()
    for copy in wcopies:
        copy.wait()

    arrive(0, 0, GROUP)
    interleave(encode(0))
    gather(1)

    def consume(c, carry):
        arrive(c, c * GROUP, GROUP)
        interleave(route(c - 1), encode(c))
        gather(c + 1)

        @pl.when(c > 1)
        def _():
            exchange(c - 2).start()

        return carry

    last = chunks - 1
    lax.fori_loop(1, last, consume, 0)
    interleave(route(last - 1))
    exchange(last - 2).start()
    arrive(last, *pieces[last])
    interleave(encode(last, 0, part))
    exchange(last - 1).start()
    arrive(chunks, *pieces[chunks])
    interleave(encode(last, part, part))
    interleave(route(last))
    exchange(last).start()

    def drain(c, carry):
        exchange(c).wait()
        for step in range(n - 1):
            send_of(c, c * GROUP, GROUP, step).wait_send()
        return carry

    for step in range(n - 1):
        send_ids(step).wait_send()
        for p in (chunks - 1, chunks):
            send_of(p, *pieces[p], step).wait_send()
    lax.fori_loop(0, last, drain, 0)
    exchange(last).wait()


def body(
    features, item_ids, item_table, lengths, routing_seed, w_qkv, w_out, w_bilinear, w_up, w_down
):
    n = lax.axis_size("pa")
    cores = lax.axis_size("dev")
    span, width = features.shape[1:]
    owned = lengths.shape[0] // n
    share = owned // cores
    history = n * span
    if (
        cores != 2 or span % 16 or share % 128 or n < 2 or history * HEADS != width
        or item_table.shape[0] % 256
    ):
        return plain_body(
            features, item_ids, item_table, lengths, routing_seed,
            w_qkv, w_out, w_bilinear, w_up, w_down,
        )
    chunks = share // GROUP
    rows = GROUP * history
    ff = w_up.shape[1] * cores
    hbm = pl.BlockSpec(memory_space=pltpu.HBM)
    vmem = pl.BlockSpec(memory_space=pltpu.VMEM)
    smem = pl.BlockSpec(memory_space=pltpu.SMEM)
    dma = pltpu.SemaphoreType.DMA
    routed = pl.pallas_call(
        functools.partial(fused, n, share),
        out_shape=jax.ShapeDtypeStruct((owned * CAPS, width // cores), F32),
        in_specs=[hbm, smem, hbm, hbm, vmem] + [hbm] * 5,
        out_specs=vmem,
        scratch_shapes=[
            pltpu.VMEM((share, history, width), BF16),
            pltpu.VMEM((n, span, share), jnp.int32),
            pltpu.SMEM((n, span, share), jnp.int32),
            pltpu.VMEM(item_table.shape, BF16),
            pltpu.VMEM((item_table.shape[0] * 2, width // 2), F32),
            pltpu.VMEM((rows * 2, width // 2), F32),
            pltpu.VMEM((rows, width), BF16),
            pltpu.VMEM((CAPS * GROUP, rows), F32),
            pltpu.VMEM((width, 3 * width + ff), BF16),
            pltpu.VMEM((2 * width + ff, width), BF16),
            pltpu.VMEM((HEADS * history, width), BF16),
            pltpu.VMEM((rows, 3 * width), BF16),
            pltpu.VMEM((rows, width + ff), BF16),
            pltpu.VMEM((rows, width), BF16),
            pltpu.VMEM((rows, width), BF16),
            pltpu.VMEM((rows, width), F32),
            pltpu.VMEM((2, rows, width), BF16),
            pltpu.VMEM((share * CAPS, width // cores), F32),
            dma, dma, dma((2,)), dma((n - 1,)), dma((n - 1,)), dma((7,)), dma((7,)), dma((7,)),
            dma((chunks + 1, n - 1)), dma((chunks + 1, n - 1)), dma((chunks,)), dma((chunks,)),
        ],
        compiler_params=pltpu.CompilerParams(
            collective_id=0, has_side_effects=True, vmem_limit_bytes=VMEM_LIMIT
        ),
        name="encode_route",
    )(
        item_ids.T, lengths, features, item_table, routing_seed,
        w_qkv, w_out, w_bilinear, w_up, w_down,
    )
    return routed.reshape(owned, CAPS, width // cores)


VMEM_LIMIT = 60 * 1024 * 1024


def solution(mesh):
    in_specs = (
        P("au", "pa", None),
        P("au", "pa"),
        P(),
        P("au"),
        P(),
        P(None, None, "dev"),
        P("dev", None),
        P(None, "dev"),
        P(None, "dev"),
        P("dev", None),
    )
    out_specs = P(("au", "pa"), None, "dev")
    return jax.shard_map(body, mesh=mesh, in_specs=in_specs, out_specs=out_specs, check_vma=False)
```

```python
import functools

import jax
import jax.numpy as jnp
from jax import lax
from jax.experimental import pallas as pl
from jax.experimental.pallas import tpu as pltpu
from jax.sharding import PartitionSpec as P

D = 256
HEADS = 4
CAPS = 4
ITERS = 3


def local_routing(vectors, valid, base):
    user_count, history_len, width_here = vectors.shape
    logits = jnp.broadcast_to(base[None], (user_count, CAPS, history_len))
    capsules = jnp.zeros((user_count, CAPS, width_here), jnp.float32)
    for sweep in range(ITERS):
        weights = jax.nn.softmax(logits, axis=1) * valid[:, None, :]
        summed = jnp.einsum("ukl,uld->ukd", weights, vectors, precision=lax.Precision.HIGHEST)
        squares = jnp.sum(summed * summed, axis=-1)
        factor = jnp.sqrt(squares) / (1.0 + squares)
        capsules = summed * factor[..., None]
        if sweep + 1 < ITERS:
            logits = logits + jnp.einsum(
                "ukd,uld->ukl", capsules, vectors, precision=lax.Precision.HIGHEST
            )
    return capsules


def plain_body(
    features, item_ids, item_table, lengths, routing_seed, w_qkv, w_out, w_bilinear, w_up, w_down
):
    pa_count = lax.axis_size("pa")
    dev_count = lax.axis_size("dev")
    owned_users = lengths.shape[0] // pa_count
    head_size = D // HEADS
    share = owned_users // dev_count
    core = lax.axis_index("dev")

    def pick(array):
        shaped = array.reshape((pa_count, dev_count, share) + array.shape[1:])
        chosen = lax.dynamic_index_in_dim(shaped, core, 1, keepdims=False)
        return chosen.reshape((pa_count * share,) + array.shape[1:])

    features = pick(features)
    item_ids = pick(item_ids)
    lengths = pick(lengths)
    w_qkv, w_out, w_bilinear, w_up, w_down = (
        lax.all_gather(w_qkv, "dev", axis=2, tiled=True),
        lax.all_gather(w_out, "dev", axis=0, tiled=True),
        lax.all_gather(w_bilinear, "dev", axis=1, tiled=True),
        lax.all_gather(w_up, "dev", axis=1, tiled=True),
        lax.all_gather(w_down, "dev", axis=0, tiled=True),
    )
    own_lens = lax.dynamic_slice_in_dim(lengths, lax.axis_index("pa") * share, share)
    features, item_ids = (
        lax.all_to_all(features, "pa", split_axis=0, concat_axis=1, tiled=True),
        lax.all_to_all(item_ids, "pa", split_axis=0, concat_axis=1, tiled=True),
    )
    user_count, span_here, model_width = features.shape
    heads_here = w_qkv.shape[2] // head_size
    inputs = (
        features.astype(jnp.float32) + jnp.take(item_table, item_ids, axis=0).astype(jnp.float32)
    ).astype(jnp.bfloat16)
    flat_rows = inputs.reshape(-1, model_width)

    def project(index):
        shaped = w_qkv[index].reshape(model_width, heads_here, head_size)
        made = jnp.einsum(
            "nd,dhe->hne", flat_rows, shaped, preferred_element_type=jnp.float32
        ).astype(jnp.bfloat16)
        return made.reshape(heads_here, user_count, span_here, head_size)

    queries = project(0)
    key_block = project(1)
    value_block = project(2)
    score_scale = 1.0 / head_size**0.5
    count_here = key_block.shape[2]
    scores = (
        jnp.einsum("huqe,huke->huqk", queries, key_block, preferred_element_type=jnp.float32)
        * score_scale
    )
    positions = jnp.arange(count_here, dtype=jnp.int32)
    valid_keys = positions[None, :] < own_lens[:, None]
    mask_four = valid_keys[None, :, None, :]
    probs = jnp.where(mask_four, jnp.exp(scores), 0.0)
    totals = jnp.sum(probs, axis=-1)
    weighted = jnp.einsum(
        "huqk,huke->huqe",
        probs.astype(jnp.bfloat16),
        value_block,
        preferred_element_type=jnp.float32,
    )
    attended = (weighted / totals[..., None]).astype(jnp.bfloat16)
    out_heads = w_out.reshape(heads_here, head_size, w_out.shape[1])
    attended_term = jnp.einsum(
        "huqe,hef->uqf", attended, out_heads, preferred_element_type=jnp.float32
    )
    hidden = jax.nn.gelu(jnp.dot(flat_rows, w_up, preferred_element_type=jnp.float32)).astype(
        jnp.bfloat16
    )
    partial_terms = attended_term.reshape(-1, w_out.shape[1]) + jnp.dot(
        hidden, w_down, preferred_element_type=jnp.float32
    )
    interest_in = (
        partial_terms + jnp.dot(flat_rows, w_bilinear, preferred_element_type=jnp.float32)
    ).astype(jnp.bfloat16)
    interest_in = interest_in.reshape(user_count, span_here, -1)
    history_len = interest_in.shape[1]
    valid = (jnp.arange(history_len)[None, :] < own_lens[:, None]).astype(jnp.float32)
    base = (routing_seed.astype(jnp.float32) - 7.5) * 0.25
    routed = local_routing(interest_in.astype(jnp.float32), valid, base)
    capsules = lax.all_to_all(routed, "dev", split_axis=2, concat_axis=0, tiled=True)
    return capsules


GROUP = 8
F32, BF16 = jnp.float32, jnp.bfloat16
NT = (((1,), (1,)), ((), ()))
MESH = pl.DeviceIdType.MESH


def dot(a, b):
    return jnp.dot(a, b, preferred_element_type=F32)


def split(a):
    high = a.astype(BF16)
    low = (a - high.astype(F32)).astype(BF16)
    return jnp.concatenate([high, low], axis=0)


def interleave(*parts):
    parts = list(parts)
    while parts:
        for part in list(parts):
            try:
                next(part)
            except StopIteration:
                parts.remove(part)


def fused(
    n, share, ids, lens_in, feats, table, seed_in, w_qkv, w_out, w_bil, w_up, w_down,
    out, stage, recv, lens, seed, ids_vmem, ids_smem, table_in, table_wide, rows, x_ref, base, w_in, w_mix, blocks,
    qkv, mix, high, low, weighted, interests, outbox,
    table_sem, own_sem, feat_sem, small_sem, id_sem, idsend_sem, idrecv_sem, wown_sem, wsend_sem, wrecv_sem,
    send_sem, recv_sem, xsend_sem, xrecv_sem,
):
    me = lax.axis_index("pa")
    core = lax.axis_index("dev")
    sibling = 1 - core
    span, width = feats.shape[1], feats.shape[2]
    history = n * span
    head = width // HEADS
    half = width // 2
    chunks = share // GROUP
    part = GROUP // 2
    pieces = [(c * GROUP, GROUP) for c in range(chunks - 1)]
    pieces += [(share - GROUP, part), (share - part, part)]

    def owner(step):
        return lax.rem(me + step + 1, n)

    def first_user(who):
        return pl.multiple_of((who * 2 + core) * share, share)

    barrier = pltpu.get_barrier_semaphore()
    for step in range(n - 1):
        pl.semaphore_signal(barrier, inc=1, device_id={"pa": owner(step)}, device_id_type=MESH)
    pl.semaphore_signal(barrier, inc=1, device_id={"dev": sibling}, device_id_type=MESH)

    feat_copies = []
    for step in range(n - 1):
        copy = pltpu.make_async_copy(
            feats.at[pl.ds(first_user(owner(step)), share)], stage.at[step], feat_sem.at[step]
        )
        copy.start()
        feat_copies.append(copy)
    table_copy = pltpu.make_async_copy(table, table_in, table_sem)
    table_copy.start()
    small_copies = [
        pltpu.make_async_copy(lens_in, lens, small_sem.at[0]),
        pltpu.make_async_copy(seed_in, seed, small_sem.at[1]),
    ]
    for copy in small_copies:
        copy.start()
    own_feats = pltpu.make_async_copy(
        feats.at[pl.ds(first_user(me), share)],
        recv.at[:, pl.ds(pl.multiple_of(me * span, span), span), :],
        own_sem,
    )
    own_feats.start()
    own_ids = pltpu.make_async_copy(
        ids.at[:, pl.ds(first_user(me), share)], ids_vmem.at[me], id_sem.at[0]
    )
    own_ids.start()

    up_half = w_up.shape[1]
    down_half = w_down.shape[0]

    def cols(start, size):
        return pl.ds(pl.multiple_of(start, 128), size)

    weights = [
        (w_qkv.at[i], w_in.at[:, cols(i * width + core * half, half)]) for i in range(3)
    ] + [
        (w_up, w_in.at[:, cols(3 * width + core * up_half, up_half)]),
        (w_bil, w_mix.at[pl.ds(0, width), cols(core * half, half)]),
        (w_out, w_mix.at[cols(width + core * half, half), :]),
        (w_down, w_mix.at[cols(2 * width + core * down_half, down_half), :]),
    ]
    own_copies = []
    for i, (source, target) in enumerate(weights):
        copy = pltpu.make_async_copy(source, target, wown_sem.at[i])
        copy.start()
        own_copies.append(copy)

    def send_ids(step):
        return pltpu.make_async_remote_copy(
            ids.at[:, pl.ds(first_user(owner(step)), share)],
            ids_vmem.at[me],
            idsend_sem.at[step],
            idrecv_sem.at[step],
            device_id={"pa": owner(step)},
            device_id_type=MESH,
        )

    def send_of(p, start, size, step):
        return pltpu.make_async_remote_copy(
            stage.at[step, pl.ds(start, size)],
            recv.at[pl.ds(start, size), pl.ds(pl.multiple_of(me * span, span), span), :],
            send_sem.at[p, step],
            recv_sem.at[p, step],
            device_id={"pa": owner(step)},
            device_id_type=MESH,
        )

    wcopies = []
    for i, (source, target) in enumerate(weights):
        wcopies.append(
            pltpu.make_async_remote_copy(
                source, target, wsend_sem.at[i], wrecv_sem.at[i],
                device_id={"dev": sibling}, device_id_type=MESH,
            )
        )

    for copy in feat_copies:
        copy.wait()
    pl.semaphore_wait(barrier, n)
    for step in range(n - 1):
        send_ids(step).start()

    def launch(c, carry):
        for step in range(n - 1):
            send_of(c, c * GROUP, GROUP, step).start()
        return carry

    launch(0, 0)
    for copy in wcopies:
        copy.start()
    lax.fori_loop(1, AHEAD, launch, 0)

    for copy in small_copies:
        copy.wait()
    base_here = (seed[...].astype(F32) - 7.5) * 0.25
    base_here = jnp.concatenate([base_here] * GROUP, axis=1)
    for j in range(CAPS):
        base[j * GROUP : (j + 1) * GROUP, :] = jnp.broadcast_to(
            base_here[j : j + 1], (GROUP, GROUP * history)
        )
    blocks[...] = (
        lax.broadcasted_iota(jnp.int32, blocks.shape, 0) // history
        == lax.broadcasted_iota(jnp.int32, blocks.shape, 1) // head
    ).astype(F32).astype(BF16)

    table_copy.wait()

    def widen(i, carry):
        at = pl.ds(pl.multiple_of(i * 256, 256), 256)
        for h in range(2):
            table_wide[pl.ds(pl.multiple_of(i * 512, 512) + h, 256, stride=2), :] = table_in[
                at, h * half : (h + 1) * half
            ].astype(F32)
        return carry

    lax.fori_loop(0, table_in.shape[0] // 256, widen, 0)

    own_ids.wait()
    for step in range(n - 1):
        send_ids(step).wait_recv()
    id_copy = pltpu.make_async_copy(ids_vmem, ids_smem, id_sem.at[1])
    id_copy.start()
    id_copy.wait()

    def gather(c):
        def fetch(u, carry):
            for z in range(n):
                for p in range(span):
                    spot = pl.multiple_of(u * 2 * history, 2 * history) + 2 * (z * span + p)
                    rows[pl.ds(spot, 2), :] = table_wide[
                        pl.ds(ids_smem[z, p, c * GROUP + u] * 2, 2), :
                    ]
            return carry

        lax.fori_loop(0, GROUP, fetch, 0)

    ff = w_in.shape[1] - 3 * width
    span_rows = GROUP * history
    lane = lax.broadcasted_iota(jnp.int32, (history, HEADS * history), 1)
    key_spot = lax.rem(lane, history)

    def lengths_of(g):
        length_at = (me * 2 + core) * share + g * GROUP
        return [lens[length_at + u] for u in range(GROUP)]

    def encode(g, first=0, users=GROUP):
        lengths = lengths_of(g)
        span_here = slice(first * history, (first + users) * history)
        count = users * history
        feats_here = recv[pl.ds(g * GROUP + first, users)].reshape(count, width)
        for h in range(2):
            columns = slice(h * half, (h + 1) * half)
            x_ref[span_here, columns] = (
                feats_here[:, columns].astype(F32)
                + rows[pl.ds(2 * first * history + h, count, stride=2), :]
            ).astype(BF16)
        x = x_ref[span_here, :]
        for f in range(0, 3 * width, width):
            qkv[span_here, f : f + width] = dot(x, w_in[:, f : f + width]).astype(BF16)
            yield
        ats = [(u, pl.ds(u * history, history)) for u in range(first, first + users)]
        for u, at in ats:
            keys = jnp.concatenate([qkv[at, width : 2 * width]] * HEADS, axis=0) * blocks[...]
            scores = lax.dot_general(
                qkv[at, :width], keys, NT, preferred_element_type=F32
            ) * (1.0 / head**0.5)
            probs = jnp.where(key_spot < lengths[u], jnp.exp(scores), 0.0)
            top = probs.astype(BF16)
            high[at, :] = top
            low[at, :] = (probs - top.astype(F32)).astype(BF16)
            if u % 2:
                yield
        for f in range(0, ff, 256):
            up = dot(x, w_in[:, 3 * width + f : 3 * width + f + 256])
            mix[span_here, width + f : width + f + 256] = jax.nn.gelu(up).astype(BF16)
            yield
        for u, at in ats:
            values = jnp.concatenate([qkv[at, 2 * width :]] * HEADS, axis=0) * blocks[...]
            weighted[at, :] = dot(high[at, :], values)
            if u % 2:
                yield
        totals = dot(high[span_here, :], blocks[...]) + dot(low[span_here, :], blocks[...])
        mix[span_here, :width] = (weighted[span_here, :] / totals).astype(BF16)
        yield
        made = (dot(x, w_mix[:width, :]) + dot(mix[span_here, :], w_mix[width:, :])).astype(BF16)
        interests[lax.rem(g, 2), span_here, :] = made

    def route(g):
        lengths = lengths_of(g)
        slot = lax.rem(g, 2)
        row = lax.broadcasted_iota(jnp.int32, (GROUP, span_rows), 0)
        col = lax.broadcasted_iota(jnp.int32, (GROUP, span_rows), 1)
        limit = jnp.zeros((GROUP, span_rows), jnp.int32)
        for u in range(GROUP):
            limit = jnp.where(row == u, u * history + lengths[u], limit)
        valid = ((col >= row * history) & (col < limit)).astype(F32)
        logits = [base[j * GROUP : (j + 1) * GROUP, :] for j in range(CAPS)]
        capsules = None
        for sweep in range(ITERS):
            peak = functools.reduce(jnp.maximum, logits)
            powers = [jnp.exp(l - peak) for l in logits]
            scale = valid / functools.reduce(jnp.add, powers)
            weights_here = jnp.concatenate([p * scale for p in powers], axis=0)
            both = dot(split(weights_here), interests[slot])
            yield
            yield
            summed = both[: CAPS * GROUP] + both[CAPS * GROUP :]
            squares = jnp.sum(summed * summed, axis=1, keepdims=True)
            yield
            capsules = summed * (jnp.sqrt(squares) / (1.0 + squares))
            if sweep + 1 < ITERS:
                both = lax.dot_general(
                    split(capsules), interests[slot], NT, preferred_element_type=F32
                )
                yield
                yield
                gain = both[: CAPS * GROUP] + both[CAPS * GROUP :]
                logits = [
                    l + gain[j * GROUP : (j + 1) * GROUP] for j, l in enumerate(logits)
                ]
        mine = jnp.where(core == 0, capsules[:, :half], capsules[:, half:])
        theirs = jnp.where(core == 0, capsules[:, half:], capsules[:, :half])
        first = g * GROUP * CAPS
        for j in range(CAPS):
            here = slice(j * GROUP, (j + 1) * GROUP)
            spot = pl.multiple_of(core * share * CAPS + first, GROUP * CAPS) + j
            out[pl.ds(spot, GROUP, stride=CAPS), :] = mine[here]
            spot = pl.multiple_of(first, GROUP * CAPS) + j
            outbox[pl.ds(spot, GROUP, stride=CAPS), :] = theirs[here]

    size = GROUP * CAPS

    def exchange(c):
        return pltpu.make_async_remote_copy(
            outbox.at[pl.ds(pl.multiple_of(c * size, size), size), :],
            out.at[pl.ds(pl.multiple_of(core * share * CAPS + c * size, size), size), :],
            xsend_sem.at[c],
            xrecv_sem.at[c],
            device_id={"dev": sibling},
            device_id_type=MESH,
        )

    def arrive(p, start, size):
        for step in range(n - 1):
            send_of(p, start, size, step).wait_recv()

    gather(0)
    own_feats.wait()
    for copy in own_copies:
        copy.wait()
    for copy in wcopies:
        copy.wait()

    def advance(c):
        @pl.when(c + AHEAD < chunks - 1)
        def _():
            launch(c + AHEAD, 0)

        @pl.when(c + AHEAD == chunks - 1)
        def _():
            for p in (chunks - 1, chunks):
                for step in range(n - 1):
                    send_of(p, *pieces[p], step).start()

    arrive(0, 0, GROUP)
    advance(0)
    interleave(encode(0))
    gather(1)

    def consume(c, carry):
        arrive(c, c * GROUP, GROUP)
        advance(c)
        interleave(route(c - 1), encode(c))
        gather(c + 1)

        @pl.when(c > 1)
        def _():
            exchange(c - 2).start()

        return carry

    last = chunks - 1
    lax.fori_loop(1, last, consume, 0)
    interleave(route(last - 1))
    exchange(last - 2).start()
    arrive(last, *pieces[last])
    interleave(encode(last, 0, part))
    exchange(last - 1).start()
    arrive(chunks, *pieces[chunks])
    interleave(encode(last, part, part))
    interleave(route(last))
    exchange(last).start()

    def drain(c, carry):
        exchange(c).wait()
        for step in range(n - 1):
            send_of(c, c * GROUP, GROUP, step).wait_send()
        return carry

    for step in range(n - 1):
        send_ids(step).wait_send()
        for p in (chunks - 1, chunks):
            send_of(p, *pieces[p], step).wait_send()
    lax.fori_loop(0, last, drain, 0)
    exchange(last).wait()


def body(
    features, item_ids, item_table, lengths, routing_seed, w_qkv, w_out, w_bilinear, w_up, w_down
):
    n = lax.axis_size("pa")
    cores = lax.axis_size("dev")
    span, width = features.shape[1:]
    owned = lengths.shape[0] // n
    share = owned // cores
    history = n * span
    if (
        cores != 2 or span % 16 or share % 128 or n < 2 or history * HEADS != width
        or item_table.shape[0] % 256
    ):
        return plain_body(
            features, item_ids, item_table, lengths, routing_seed,
            w_qkv, w_out, w_bilinear, w_up, w_down,
        )
    chunks = share // GROUP
    rows = GROUP * history
    ff = w_up.shape[1] * cores
    hbm = pl.BlockSpec(memory_space=pltpu.HBM)
    vmem = pl.BlockSpec(memory_space=pltpu.VMEM)
    dma = pltpu.SemaphoreType.DMA
    routed = pl.pallas_call(
        functools.partial(fused, n, share),
        out_shape=jax.ShapeDtypeStruct((owned * CAPS, width // cores), F32),
        in_specs=[hbm] * 10,
        out_specs=vmem,
        scratch_shapes=[
            pltpu.VMEM((n - 1, share, span, width), BF16),
            pltpu.VMEM((share, history, width), BF16),
            pltpu.SMEM(lengths.shape, jnp.int32),
            pltpu.VMEM(routing_seed.shape, jnp.int32),
            pltpu.VMEM((n, span, share), jnp.int32),
            pltpu.SMEM((n, span, share), jnp.int32),
            pltpu.VMEM(item_table.shape, BF16),
            pltpu.VMEM((item_table.shape[0] * 2, width // 2), F32),
            pltpu.VMEM((rows * 2, width // 2), F32),
            pltpu.VMEM((rows, width), BF16),
            pltpu.VMEM((CAPS * GROUP, rows), F32),
            pltpu.VMEM((width, 3 * width + ff), BF16),
            pltpu.VMEM((2 * width + ff, width), BF16),
            pltpu.VMEM((HEADS * history, width), BF16),
            pltpu.VMEM((rows, 3 * width), BF16),
            pltpu.VMEM((rows, width + ff), BF16),
            pltpu.VMEM((rows, width), BF16),
            pltpu.VMEM((rows, width), BF16),
            pltpu.VMEM((rows, width), F32),
            pltpu.VMEM((2, rows, width), BF16),
            pltpu.VMEM((share * CAPS, width // cores), F32),
            dma, dma, dma((n - 1,)), dma((2,)), dma((2,)), dma((n - 1,)), dma((n - 1,)), dma((7,)), dma((7,)), dma((7,)),
            dma((chunks + 1, n - 1)), dma((chunks + 1, n - 1)), dma((chunks,)), dma((chunks,)),
        ],
        compiler_params=pltpu.CompilerParams(
            collective_id=0, has_side_effects=True, vmem_limit_bytes=VMEM_LIMIT
        ),
        name="encode_route",
    )(*(pltpu.with_memory_space_constraint(a, pltpu.HBM) for a in (
        item_ids.T, lengths, features, item_table, routing_seed,
        w_qkv, w_out, w_bilinear, w_up, w_down,
    )))
    return routed.reshape(owned, CAPS, width // cores)


AHEAD = 2
VMEM_LIMIT = 50 * 1024 * 1024


def solution(mesh):
    in_specs = (
        P("au", "pa", None),
        P("au", "pa"),
        P(),
        P("au"),
        P(),
        P(None, None, "dev"),
        P("dev", None),
        P(None, "dev"),
        P(None, "dev"),
        P("dev", None),
    )
    out_specs = P(("au", "pa"), None, "dev")
    return jax.shard_map(body, mesh=mesh, in_specs=in_specs, out_specs=out_specs, check_vma=False)
```

```python
import functools

import jax
import jax.numpy as jnp
from jax import lax
from jax.experimental import pallas as pl
from jax.experimental.pallas import tpu as pltpu
from jax.sharding import PartitionSpec as P

D = 256
HEADS = 4
CAPS = 4
ITERS = 3


def local_routing(vectors, valid, base):
    user_count, history_len, width_here = vectors.shape
    logits = jnp.broadcast_to(base[None], (user_count, CAPS, history_len))
    capsules = jnp.zeros((user_count, CAPS, width_here), jnp.float32)
    for sweep in range(ITERS):
        weights = jax.nn.softmax(logits, axis=1) * valid[:, None, :]
        summed = jnp.einsum("ukl,uld->ukd", weights, vectors, precision=lax.Precision.HIGHEST)
        squares = jnp.sum(summed * summed, axis=-1)
        factor = jnp.sqrt(squares) / (1.0 + squares)
        capsules = summed * factor[..., None]
        if sweep + 1 < ITERS:
            logits = logits + jnp.einsum(
                "ukd,uld->ukl", capsules, vectors, precision=lax.Precision.HIGHEST
            )
    return capsules


def plain_body(
    features, item_ids, item_table, lengths, routing_seed, w_qkv, w_out, w_bilinear, w_up, w_down
):
    pa_count = lax.axis_size("pa")
    dev_count = lax.axis_size("dev")
    owned_users = lengths.shape[0] // pa_count
    head_size = D // HEADS
    share = owned_users // dev_count
    core = lax.axis_index("dev")

    def pick(array):
        shaped = array.reshape((pa_count, dev_count, share) + array.shape[1:])
        chosen = lax.dynamic_index_in_dim(shaped, core, 1, keepdims=False)
        return chosen.reshape((pa_count * share,) + array.shape[1:])

    features = pick(features)
    item_ids = pick(item_ids)
    lengths = pick(lengths)
    w_qkv, w_out, w_bilinear, w_up, w_down = (
        lax.all_gather(w_qkv, "dev", axis=2, tiled=True),
        lax.all_gather(w_out, "dev", axis=0, tiled=True),
        lax.all_gather(w_bilinear, "dev", axis=1, tiled=True),
        lax.all_gather(w_up, "dev", axis=1, tiled=True),
        lax.all_gather(w_down, "dev", axis=0, tiled=True),
    )
    own_lens = lax.dynamic_slice_in_dim(lengths, lax.axis_index("pa") * share, share)
    features, item_ids = (
        lax.all_to_all(features, "pa", split_axis=0, concat_axis=1, tiled=True),
        lax.all_to_all(item_ids, "pa", split_axis=0, concat_axis=1, tiled=True),
    )
    user_count, span_here, model_width = features.shape
    heads_here = w_qkv.shape[2] // head_size
    inputs = (
        features.astype(jnp.float32) + jnp.take(item_table, item_ids, axis=0).astype(jnp.float32)
    ).astype(jnp.bfloat16)
    flat_rows = inputs.reshape(-1, model_width)

    def project(index):
        shaped = w_qkv[index].reshape(model_width, heads_here, head_size)
        made = jnp.einsum(
            "nd,dhe->hne", flat_rows, shaped, preferred_element_type=jnp.float32
        ).astype(jnp.bfloat16)
        return made.reshape(heads_here, user_count, span_here, head_size)

    queries = project(0)
    key_block = project(1)
    value_block = project(2)
    score_scale = 1.0 / head_size**0.5
    count_here = key_block.shape[2]
    scores = (
        jnp.einsum("huqe,huke->huqk", queries, key_block, preferred_element_type=jnp.float32)
        * score_scale
    )
    positions = jnp.arange(count_here, dtype=jnp.int32)
    valid_keys = positions[None, :] < own_lens[:, None]
    mask_four = valid_keys[None, :, None, :]
    probs = jnp.where(mask_four, jnp.exp(scores), 0.0)
    totals = jnp.sum(probs, axis=-1)
    weighted = jnp.einsum(
        "huqk,huke->huqe",
        probs.astype(jnp.bfloat16),
        value_block,
        preferred_element_type=jnp.float32,
    )
    attended = (weighted / totals[..., None]).astype(jnp.bfloat16)
    out_heads = w_out.reshape(heads_here, head_size, w_out.shape[1])
    attended_term = jnp.einsum(
        "huqe,hef->uqf", attended, out_heads, preferred_element_type=jnp.float32
    )
    hidden = jax.nn.gelu(jnp.dot(flat_rows, w_up, preferred_element_type=jnp.float32)).astype(
        jnp.bfloat16
    )
    partial_terms = attended_term.reshape(-1, w_out.shape[1]) + jnp.dot(
        hidden, w_down, preferred_element_type=jnp.float32
    )
    interest_in = (
        partial_terms + jnp.dot(flat_rows, w_bilinear, preferred_element_type=jnp.float32)
    ).astype(jnp.bfloat16)
    interest_in = interest_in.reshape(user_count, span_here, -1)
    history_len = interest_in.shape[1]
    valid = (jnp.arange(history_len)[None, :] < own_lens[:, None]).astype(jnp.float32)
    base = (routing_seed.astype(jnp.float32) - 7.5) * 0.25
    routed = local_routing(interest_in.astype(jnp.float32), valid, base)
    capsules = lax.all_to_all(routed, "dev", split_axis=2, concat_axis=0, tiled=True)
    return capsules


GROUP = 8
F32, BF16 = jnp.float32, jnp.bfloat16
NT = (((1,), (1,)), ((), ()))
MESH = pl.DeviceIdType.MESH


def dot(a, b):
    return jnp.dot(a, b, preferred_element_type=F32)


def split(a):
    high = a.astype(BF16)
    low = (a - high.astype(F32)).astype(BF16)
    return jnp.concatenate([high, low], axis=0)


def interleave(*parts):
    parts = list(parts)
    while parts:
        for part in list(parts):
            try:
                next(part)
            except StopIteration:
                parts.remove(part)


def fused(
    n, share, ids, lens_in, feats, table, seed_in, w_qkv, w_out, w_bil, w_up, w_down,
    out, stage, recv, lens, seed, ids_vmem, ids_smem, table_in, table_wide, rows, x_ref, base, w_in, w_mix, blocks,
    qkv, mix, high, low, weighted, interests, outbox,
    table_sem, own_sem, feat_sem, small_sem, id_sem, idsend_sem, idrecv_sem, wown_sem, wsend_sem, wrecv_sem,
    send_sem, recv_sem, xsend_sem, xrecv_sem,
):
    me = lax.axis_index("pa")
    core = lax.axis_index("dev")
    sibling = 1 - core
    span, width = feats.shape[1], feats.shape[2]
    history = n * span
    head = width // HEADS
    half = width // 2
    chunks = share // GROUP
    part = GROUP // 2
    pieces = [(c * GROUP, GROUP) for c in range(chunks - 1)]
    pieces += [(share - GROUP, part), (share - part, part)]

    def owner(step):
        return lax.rem(me + step + 1, n)

    def first_user(who):
        return pl.multiple_of((who * 2 + core) * share, share)

    barrier = pltpu.get_barrier_semaphore()
    for step in range(n - 1):
        pl.semaphore_signal(barrier, inc=1, device_id={"pa": owner(step)}, device_id_type=MESH)
    pl.semaphore_signal(barrier, inc=1, device_id={"dev": sibling}, device_id_type=MESH)

    feat_copies = []
    for step in range(n - 1):
        copy = pltpu.make_async_copy(
            feats.at[pl.ds(first_user(owner(step)), share)], stage.at[step], feat_sem.at[step]
        )
        copy.start()
        feat_copies.append(copy)
    table_copy = pltpu.make_async_copy(table, table_in, table_sem)
    table_copy.start()
    small_copies = [
        pltpu.make_async_copy(lens_in, lens, small_sem.at[0]),
        pltpu.make_async_copy(seed_in, seed, small_sem.at[1]),
    ]
    for copy in small_copies:
        copy.start()
    own_feats = pltpu.make_async_copy(
        feats.at[pl.ds(first_user(me), share)],
        recv.at[:, pl.ds(pl.multiple_of(me * span, span), span), :],
        own_sem,
    )
    own_feats.start()
    own_ids = pltpu.make_async_copy(
        ids.at[:, pl.ds(first_user(me), share)], ids_vmem.at[me], id_sem.at[0]
    )
    own_ids.start()

    up_half = w_up.shape[1]
    down_half = w_down.shape[0]

    def cols(start, size):
        return pl.ds(pl.multiple_of(start, 128), size)

    weights = [
        (w_qkv.at[i], w_in.at[:, cols(i * width + core * half, half)]) for i in range(3)
    ] + [
        (w_up, w_in.at[:, cols(3 * width + core * up_half, up_half)]),
        (w_bil, w_mix.at[pl.ds(0, width), cols(core * half, half)]),
        (w_out, w_mix.at[cols(width + core * half, half), :]),
        (w_down, w_mix.at[cols(2 * width + core * down_half, down_half), :]),
    ]
    own_copies = []
    for i, (source, target) in enumerate(weights):
        copy = pltpu.make_async_copy(source, target, wown_sem.at[i])
        copy.start()
        own_copies.append(copy)

    def send_ids(step):
        return pltpu.make_async_remote_copy(
            ids.at[:, pl.ds(first_user(owner(step)), share)],
            ids_vmem.at[me],
            idsend_sem.at[step],
            idrecv_sem.at[step],
            device_id={"pa": owner(step)},
            device_id_type=MESH,
        )

    def send_of(p, start, size, step):
        return pltpu.make_async_remote_copy(
            stage.at[step, pl.ds(start, size)],
            recv.at[pl.ds(start, size), pl.ds(pl.multiple_of(me * span, span), span), :],
            send_sem.at[p, step],
            recv_sem.at[p, step],
            device_id={"pa": owner(step)},
            device_id_type=MESH,
        )

    wcopies = []
    for i, (source, target) in enumerate(weights):
        wcopies.append(
            pltpu.make_async_remote_copy(
                source, target, wsend_sem.at[i], wrecv_sem.at[i],
                device_id={"dev": sibling}, device_id_type=MESH,
            )
        )

    for copy in feat_copies:
        copy.wait()
    pl.semaphore_wait(barrier, n)
    for step in range(n - 1):
        send_ids(step).start()

    at_end = (me == 0) | (me == n - 1)
    lead = jnp.where(at_end, AHEAD_END, AHEAD)

    def launch(c, carry):
        for step in range(n - 1):
            send_of(c, c * GROUP, GROUP, step).start()
        return carry

    launch(0, 0)
    for copy in wcopies:
        copy.start()
    lax.fori_loop(1, lead, launch, 0)

    for copy in small_copies:
        copy.wait()
    base_here = (seed[...].astype(F32) - 7.5) * 0.25
    base_here = jnp.concatenate([base_here] * GROUP, axis=1)
    for j in range(CAPS):
        base[j * GROUP : (j + 1) * GROUP, :] = jnp.broadcast_to(
            base_here[j : j + 1], (GROUP, GROUP * history)
        )
    blocks[...] = (
        lax.broadcasted_iota(jnp.int32, blocks.shape, 0) // history
        == lax.broadcasted_iota(jnp.int32, blocks.shape, 1) // head
    ).astype(F32).astype(BF16)

    table_copy.wait()

    def widen(i, carry):
        at = pl.ds(pl.multiple_of(i * 256, 256), 256)
        for h in range(2):
            table_wide[pl.ds(pl.multiple_of(i * 512, 512) + h, 256, stride=2), :] = table_in[
                at, h * half : (h + 1) * half
            ].astype(F32)
        return carry

    lax.fori_loop(0, table_in.shape[0] // 256, widen, 0)

    own_ids.wait()
    for step in range(n - 1):
        send_ids(step).wait_recv()
    id_copy = pltpu.make_async_copy(ids_vmem, ids_smem, id_sem.at[1])
    id_copy.start()
    id_copy.wait()

    def slot_of(c):
        return pl.multiple_of(lax.rem(c, 2) * 2 * GROUP * history, 2 * GROUP * history)

    def gather(c):
        held = slot_of(c)

        def fetch(u, carry):
            for z in range(n):
                for p in range(span):
                    spot = held + pl.multiple_of(u * 2 * history, 2 * history) + 2 * (z * span + p)
                    rows[pl.ds(spot, 2), :] = table_wide[
                        pl.ds(ids_smem[z, p, c * GROUP + u] * 2, 2), :
                    ]
            return carry

        lax.fori_loop(0, GROUP, fetch, 0)

    ff = w_in.shape[1] - 3 * width
    span_rows = GROUP * history
    lane = lax.broadcasted_iota(jnp.int32, (history, HEADS * history), 1)
    key_spot = lax.rem(lane, history)

    def lengths_of(g):
        length_at = (me * 2 + core) * share + g * GROUP
        return [lens[length_at + u] for u in range(GROUP)]

    def encode(g, first=0, users=GROUP):
        lengths = lengths_of(g)
        span_here = slice(first * history, (first + users) * history)
        count = users * history
        feats_here = recv[pl.ds(g * GROUP + first, users)].reshape(count, width)
        for h in range(2):
            columns = slice(h * half, (h + 1) * half)
            x_ref[span_here, columns] = (
                feats_here[:, columns].astype(F32)
                + rows[pl.ds(slot_of(g) + 2 * first * history + h, count, stride=2), :]
            ).astype(BF16)
        x = x_ref[span_here, :]
        for f in range(0, 3 * width, width):
            qkv[span_here, f : f + width] = dot(x, w_in[:, f : f + width]).astype(BF16)
            yield
        ats = [(u, pl.ds(u * history, history)) for u in range(first, first + users)]
        for u, at in ats:
            keys = jnp.concatenate([qkv[at, width : 2 * width]] * HEADS, axis=0) * blocks[...]
            scores = lax.dot_general(
                qkv[at, :width], keys, NT, preferred_element_type=F32
            ) * (1.0 / head**0.5)
            probs = jnp.where(key_spot < lengths[u], jnp.exp(scores), 0.0)
            top = probs.astype(BF16)
            high[at, :] = top
            low[at, :] = (probs - top.astype(F32)).astype(BF16)
            if u % 2:
                yield
        for f in range(0, ff, 256):
            up = dot(x, w_in[:, 3 * width + f : 3 * width + f + 256])
            mix[span_here, width + f : width + f + 256] = jax.nn.gelu(up).astype(BF16)
            yield
        for u, at in ats:
            values = jnp.concatenate([qkv[at, 2 * width :]] * HEADS, axis=0) * blocks[...]
            weighted[at, :] = dot(high[at, :], values)
            if u % 2:
                yield
        totals = dot(high[span_here, :], blocks[...]) + dot(low[span_here, :], blocks[...])
        mix[span_here, :width] = (weighted[span_here, :] / totals).astype(BF16)
        yield
        made = (dot(x, w_mix[:width, :]) + dot(mix[span_here, :], w_mix[width:, :])).astype(BF16)
        interests[lax.rem(g, 2), span_here, :] = made

    def route(g):
        lengths = lengths_of(g)
        slot = lax.rem(g, 2)
        row = lax.broadcasted_iota(jnp.int32, (GROUP, span_rows), 0)
        col = lax.broadcasted_iota(jnp.int32, (GROUP, span_rows), 1)
        limit = jnp.zeros((GROUP, span_rows), jnp.int32)
        for u in range(GROUP):
            limit = jnp.where(row == u, u * history + lengths[u], limit)
        valid = ((col >= row * history) & (col < limit)).astype(F32)
        logits = [base[j * GROUP : (j + 1) * GROUP, :] for j in range(CAPS)]
        capsules = None
        for sweep in range(ITERS):
            peak = functools.reduce(jnp.maximum, logits)
            powers = [jnp.exp(l - peak) for l in logits]
            scale = valid / functools.reduce(jnp.add, powers)
            weights_here = jnp.concatenate([p * scale for p in powers], axis=0)
            both = dot(split(weights_here), interests[slot])
            yield
            yield
            summed = both[: CAPS * GROUP] + both[CAPS * GROUP :]
            squares = jnp.sum(summed * summed, axis=1, keepdims=True)
            yield
            capsules = summed * (jnp.sqrt(squares) / (1.0 + squares))
            if sweep + 1 < ITERS:
                both = lax.dot_general(
                    split(capsules), interests[slot], NT, preferred_element_type=F32
                )
                yield
                yield
                gain = both[: CAPS * GROUP] + both[CAPS * GROUP :]
                logits = [
                    l + gain[j * GROUP : (j + 1) * GROUP] for j, l in enumerate(logits)
                ]
        mine = jnp.where(core == 0, capsules[:, :half], capsules[:, half:])
        theirs = jnp.where(core == 0, capsules[:, half:], capsules[:, :half])
        first = g * GROUP * CAPS
        for j in range(CAPS):
            here = slice(j * GROUP, (j + 1) * GROUP)
            spot = pl.multiple_of(core * share * CAPS + first, GROUP * CAPS) + j
            out[pl.ds(spot, GROUP, stride=CAPS), :] = mine[here]
            spot = pl.multiple_of(first, GROUP * CAPS) + j
            outbox[pl.ds(spot, GROUP, stride=CAPS), :] = theirs[here]

    size = GROUP * CAPS

    def exchange(c):
        return pltpu.make_async_remote_copy(
            outbox.at[pl.ds(pl.multiple_of(c * size, size), size), :],
            out.at[pl.ds(pl.multiple_of(core * share * CAPS + c * size, size), size), :],
            xsend_sem.at[c],
            xrecv_sem.at[c],
            device_id={"dev": sibling},
            device_id_type=MESH,
        )

    def arrive(p, start, size):
        for step in range(n - 1):
            send_of(p, start, size, step).wait_recv()

    gather(0)
    own_feats.wait()
    for copy in own_copies:
        copy.wait()
    for copy in wcopies:
        copy.wait()

    def advance(c):
        @pl.when(c + lead < chunks - 1)
        def _():
            launch(c + lead, 0)

        @pl.when(c + lead == chunks - 1)
        def _():
            for p in (chunks - 1, chunks):
                for step in range(n - 1):
                    send_of(p, *pieces[p], step).start()

    gather(1)
    arrive(0, 0, GROUP)
    advance(0)
    interleave(encode(0))

    def consume(c, carry):
        gather(c + 1)
        arrive(c, c * GROUP, GROUP)
        advance(c)
        interleave(route(c - 1), encode(c))

        @pl.when(c > 1)
        def _():
            exchange(c - 2).start()

        return carry

    last = chunks - 1
    lax.fori_loop(1, last - 1, consume, 0)
    exchange(last - 3).start()
    gather(last)
    interleave(route(last - 2))
    arrive(last - 1, (last - 1) * GROUP, GROUP)
    interleave(encode(last - 1))
    exchange(last - 2).start()
    arrive(last, *pieces[last])
    interleave(encode(last, 0, part))
    arrive(chunks, *pieces[chunks])
    interleave(route(last - 1), encode(last, part, part))
    exchange(last - 1).start()
    interleave(route(last))
    exchange(last).start()

    def drain(c, carry):
        exchange(c).wait()
        for step in range(n - 1):
            send_of(c, c * GROUP, GROUP, step).wait_send()
        return carry

    for step in range(n - 1):
        send_ids(step).wait_send()
        for p in (chunks - 1, chunks):
            send_of(p, *pieces[p], step).wait_send()
    lax.fori_loop(0, last, drain, 0)
    exchange(last).wait()


def body(
    features, item_ids, item_table, lengths, routing_seed, w_qkv, w_out, w_bilinear, w_up, w_down
):
    n = lax.axis_size("pa")
    cores = lax.axis_size("dev")
    span, width = features.shape[1:]
    owned = lengths.shape[0] // n
    share = owned // cores
    history = n * span
    if (
        cores != 2 or span % 16 or share % 128 or n < 2 or share < 4 * GROUP or history * HEADS != width
        or item_table.shape[0] % 256
    ):
        return plain_body(
            features, item_ids, item_table, lengths, routing_seed,
            w_qkv, w_out, w_bilinear, w_up, w_down,
        )
    chunks = share // GROUP
    rows = GROUP * history
    ff = w_up.shape[1] * cores
    hbm = pl.BlockSpec(memory_space=pltpu.HBM)
    vmem = pl.BlockSpec(memory_space=pltpu.VMEM)
    dma = pltpu.SemaphoreType.DMA
    routed = pl.pallas_call(
        functools.partial(fused, n, share),
        out_shape=jax.ShapeDtypeStruct((owned * CAPS, width // cores), F32),
        in_specs=[hbm] * 10,
        out_specs=vmem,
        scratch_shapes=[
            pltpu.VMEM((n - 1, share, span, width), BF16),
            pltpu.VMEM((share, history, width), BF16),
            pltpu.SMEM(lengths.shape, jnp.int32),
            pltpu.VMEM(routing_seed.shape, jnp.int32),
            pltpu.VMEM((n, span, share), jnp.int32),
            pltpu.SMEM((n, span, share), jnp.int32),
            pltpu.VMEM(item_table.shape, BF16),
            pltpu.VMEM((item_table.shape[0] * 2, width // 2), F32),
            pltpu.VMEM((2 * rows * 2, width // 2), F32),
            pltpu.VMEM((rows, width), BF16),
            pltpu.VMEM((CAPS * GROUP, rows), F32),
            pltpu.VMEM((width, 3 * width + ff), BF16),
            pltpu.VMEM((2 * width + ff, width), BF16),
            pltpu.VMEM((HEADS * history, width), BF16),
            pltpu.VMEM((rows, 3 * width), BF16),
            pltpu.VMEM((rows, width + ff), BF16),
            pltpu.VMEM((rows, width), BF16),
            pltpu.VMEM((rows, width), BF16),
            pltpu.VMEM((rows, width), F32),
            pltpu.VMEM((2, rows, width), BF16),
            pltpu.VMEM((share * CAPS, width // cores), F32),
            dma, dma, dma((n - 1,)), dma((2,)), dma((2,)), dma((n - 1,)), dma((n - 1,)), dma((7,)), dma((7,)), dma((7,)),
            dma((chunks + 1, n - 1)), dma((chunks + 1, n - 1)), dma((chunks,)), dma((chunks,)),
        ],
        compiler_params=pltpu.CompilerParams(
            collective_id=0, has_side_effects=True, vmem_limit_bytes=VMEM_LIMIT
        ),
        name="encode_route",
    )(*(pltpu.with_memory_space_constraint(a, pltpu.HBM) for a in (
        item_ids.T, lengths, features, item_table, routing_seed,
        w_qkv, w_out, w_bilinear, w_up, w_down,
    )))
    return routed.reshape(owned, CAPS, width // cores)


AHEAD = 5
AHEAD_END = 2
VMEM_LIMIT = 50 * 1024 * 1024


def solution(mesh):
    in_specs = (
        P("au", "pa", None),
        P("au", "pa"),
        P(),
        P("au"),
        P(),
        P(None, None, "dev"),
        P("dev", None),
        P(None, "dev"),
        P(None, "dev"),
        P("dev", None),
    )
    out_specs = P(("au", "pa"), None, "dev")
    return jax.shard_map(body, mesh=mesh, in_specs=in_specs, out_specs=out_specs, check_vma=False)
```

```python
import functools

import jax
import jax.numpy as jnp
from jax import lax
from jax.experimental import pallas as pl
from jax.experimental.pallas import tpu as pltpu
from jax.sharding import PartitionSpec as P

D = 256
HEADS = 4
CAPS = 4
ITERS = 3


def local_routing(vectors, valid, base):
    user_count, history_len, width_here = vectors.shape
    logits = jnp.broadcast_to(base[None], (user_count, CAPS, history_len))
    capsules = jnp.zeros((user_count, CAPS, width_here), jnp.float32)
    for sweep in range(ITERS):
        weights = jax.nn.softmax(logits, axis=1) * valid[:, None, :]
        summed = jnp.einsum("ukl,uld->ukd", weights, vectors, precision=lax.Precision.HIGHEST)
        squares = jnp.sum(summed * summed, axis=-1)
        factor = jnp.sqrt(squares) / (1.0 + squares)
        capsules = summed * factor[..., None]
        if sweep + 1 < ITERS:
            logits = logits + jnp.einsum(
                "ukd,uld->ukl", capsules, vectors, precision=lax.Precision.HIGHEST
            )
    return capsules


def plain_body(
    features, item_ids, item_table, lengths, routing_seed, w_qkv, w_out, w_bilinear, w_up, w_down
):
    pa_count = lax.axis_size("pa")
    dev_count = lax.axis_size("dev")
    owned_users = lengths.shape[0] // pa_count
    head_size = D // HEADS
    share = owned_users // dev_count
    core = lax.axis_index("dev")

    def pick(array):
        shaped = array.reshape((pa_count, dev_count, share) + array.shape[1:])
        chosen = lax.dynamic_index_in_dim(shaped, core, 1, keepdims=False)
        return chosen.reshape((pa_count * share,) + array.shape[1:])

    features = pick(features)
    item_ids = pick(item_ids)
    lengths = pick(lengths)
    w_qkv, w_out, w_bilinear, w_up, w_down = (
        lax.all_gather(w_qkv, "dev", axis=2, tiled=True),
        lax.all_gather(w_out, "dev", axis=0, tiled=True),
        lax.all_gather(w_bilinear, "dev", axis=1, tiled=True),
        lax.all_gather(w_up, "dev", axis=1, tiled=True),
        lax.all_gather(w_down, "dev", axis=0, tiled=True),
    )
    own_lens = lax.dynamic_slice_in_dim(lengths, lax.axis_index("pa") * share, share)
    features, item_ids = (
        lax.all_to_all(features, "pa", split_axis=0, concat_axis=1, tiled=True),
        lax.all_to_all(item_ids, "pa", split_axis=0, concat_axis=1, tiled=True),
    )
    user_count, span_here, model_width = features.shape
    heads_here = w_qkv.shape[2] // head_size
    inputs = (
        features.astype(jnp.float32) + jnp.take(item_table, item_ids, axis=0).astype(jnp.float32)
    ).astype(jnp.bfloat16)
    flat_rows = inputs.reshape(-1, model_width)

    def project(index):
        shaped = w_qkv[index].reshape(model_width, heads_here, head_size)
        made = jnp.einsum(
            "nd,dhe->hne", flat_rows, shaped, preferred_element_type=jnp.float32
        ).astype(jnp.bfloat16)
        return made.reshape(heads_here, user_count, span_here, head_size)

    queries = project(0)
    key_block = project(1)
    value_block = project(2)
    score_scale = 1.0 / head_size**0.5
    count_here = key_block.shape[2]
    scores = (
        jnp.einsum("huqe,huke->huqk", queries, key_block, preferred_element_type=jnp.float32)
        * score_scale
    )
    positions = jnp.arange(count_here, dtype=jnp.int32)
    valid_keys = positions[None, :] < own_lens[:, None]
    mask_four = valid_keys[None, :, None, :]
    probs = jnp.where(mask_four, jnp.exp(scores), 0.0)
    totals = jnp.sum(probs, axis=-1)
    weighted = jnp.einsum(
        "huqk,huke->huqe",
        probs.astype(jnp.bfloat16),
        value_block,
        preferred_element_type=jnp.float32,
    )
    attended = (weighted / totals[..., None]).astype(jnp.bfloat16)
    out_heads = w_out.reshape(heads_here, head_size, w_out.shape[1])
    attended_term = jnp.einsum(
        "huqe,hef->uqf", attended, out_heads, preferred_element_type=jnp.float32
    )
    hidden = jax.nn.gelu(jnp.dot(flat_rows, w_up, preferred_element_type=jnp.float32)).astype(
        jnp.bfloat16
    )
    partial_terms = attended_term.reshape(-1, w_out.shape[1]) + jnp.dot(
        hidden, w_down, preferred_element_type=jnp.float32
    )
    interest_in = (
        partial_terms + jnp.dot(flat_rows, w_bilinear, preferred_element_type=jnp.float32)
    ).astype(jnp.bfloat16)
    interest_in = interest_in.reshape(user_count, span_here, -1)
    history_len = interest_in.shape[1]
    valid = (jnp.arange(history_len)[None, :] < own_lens[:, None]).astype(jnp.float32)
    base = (routing_seed.astype(jnp.float32) - 7.5) * 0.25
    routed = local_routing(interest_in.astype(jnp.float32), valid, base)
    capsules = lax.all_to_all(routed, "dev", split_axis=2, concat_axis=0, tiled=True)
    return capsules


GROUP = 8
F32, BF16 = jnp.float32, jnp.bfloat16
NT = (((1,), (1,)), ((), ()))
MESH = pl.DeviceIdType.MESH


def dot(a, b):
    return jnp.dot(a, b, preferred_element_type=F32)


def split(a):
    high = a.astype(BF16)
    low = (a - high.astype(F32)).astype(BF16)
    return jnp.concatenate([high, low], axis=0)


def interleave(*parts):
    parts = list(parts)
    while parts:
        for part in list(parts):
            try:
                next(part)
            except StopIteration:
                parts.remove(part)


def fused(
    n, share, ids, lens_in, feats, table, seed_in, w_qkv, w_out, w_bil, w_up, w_down,
    out, stage, recv, lens, seed, ids_vmem, ids_smem, table_in, table_wide, rows, x_ref, base, w_in, w_mix, blocks,
    qkv, mix, high, low, weighted, interests, outbox,
    table_sem, own_sem, feat_sem, small_sem, id_sem, idsend_sem, idrecv_sem, wown_sem, wsend_sem, wrecv_sem,
    send_sem, recv_sem, xsend_sem, xrecv_sem,
):
    me = lax.axis_index("pa")
    core = lax.axis_index("dev")
    sibling = 1 - core
    span, width = feats.shape[1], feats.shape[2]
    history = n * span
    head = width // HEADS
    half = width // 2
    chunks = share // GROUP

    def owner(step):
        return lax.rem(me + step + 1, n)

    def first_user(who):
        return pl.multiple_of((who * 2 + core) * share, share)

    barrier = pltpu.get_barrier_semaphore()
    for step in range(n - 1):
        pl.semaphore_signal(barrier, inc=1, device_id={"pa": owner(step)}, device_id_type=MESH)
    pl.semaphore_signal(barrier, inc=1, device_id={"dev": sibling}, device_id_type=MESH)

    feat_copies = []
    for step in range(n - 1):
        copy = pltpu.make_async_copy(
            feats.at[pl.ds(first_user(owner(step)), share)], stage.at[step], feat_sem.at[step]
        )
        copy.start()
        feat_copies.append(copy)
    table_copy = pltpu.make_async_copy(table, table_in, table_sem)
    table_copy.start()
    small_copies = [
        pltpu.make_async_copy(lens_in, lens, small_sem.at[0]),
        pltpu.make_async_copy(seed_in, seed, small_sem.at[1]),
    ]
    for copy in small_copies:
        copy.start()
    own_feats = pltpu.make_async_copy(
        feats.at[pl.ds(first_user(me), share)],
        recv.at[:, pl.ds(pl.multiple_of(me * span, span), span), :],
        own_sem,
    )
    own_feats.start()
    own_ids = pltpu.make_async_copy(
        ids.at[:, pl.ds(first_user(me), share)], ids_vmem.at[me], id_sem.at[0]
    )
    own_ids.start()

    up_half = w_up.shape[1]
    down_half = w_down.shape[0]

    def cols(start, size):
        return pl.ds(pl.multiple_of(start, 128), size)

    weights = [
        (w_qkv.at[i], w_in.at[:, cols(i * width + core * half, half)]) for i in range(3)
    ] + [
        (w_up, w_in.at[:, cols(3 * width + core * up_half, up_half)]),
        (w_bil, w_mix.at[pl.ds(0, width), cols(core * half, half)]),
        (w_out, w_mix.at[cols(width + core * half, half), :]),
        (w_down, w_mix.at[cols(2 * width + core * down_half, down_half), :]),
    ]
    own_copies = []
    for i, (source, target) in enumerate(weights):
        copy = pltpu.make_async_copy(source, target, wown_sem.at[i])
        copy.start()
        own_copies.append(copy)

    def send_ids(step):
        return pltpu.make_async_remote_copy(
            ids.at[:, pl.ds(first_user(owner(step)), share)],
            ids_vmem.at[me],
            idsend_sem.at[step],
            idrecv_sem.at[step],
            device_id={"pa": owner(step)},
            device_id_type=MESH,
        )

    def send_of(p, start, size, step):
        return pltpu.make_async_remote_copy(
            stage.at[step, pl.ds(start, size)],
            recv.at[pl.ds(start, size), pl.ds(pl.multiple_of(me * span, span), span), :],
            send_sem.at[p, step],
            recv_sem.at[p, step],
            device_id={"pa": owner(step)},
            device_id_type=MESH,
        )

    wcopies = []
    for i, (source, target) in enumerate(weights):
        wcopies.append(
            pltpu.make_async_remote_copy(
                source, target, wsend_sem.at[i], wrecv_sem.at[i],
                device_id={"dev": sibling}, device_id_type=MESH,
            )
        )

    for copy in feat_copies:
        copy.wait()
    pl.semaphore_wait(barrier, n)
    for step in range(n - 1):
        send_ids(step).start()

    at_end = (me == 0) | (me == n - 1)
    lead = jnp.where(at_end, AHEAD_END, AHEAD)

    def launch(c, carry):
        for step in range(n - 1):
            send_of(c, c * GROUP, GROUP, step).start()
        return carry

    launch(0, 0)
    for copy in wcopies:
        copy.start()
    lax.fori_loop(1, lead, launch, 0)

    for copy in small_copies:
        copy.wait()
    base_here = (seed[...].astype(F32) - 7.5) * 0.25
    base_here = jnp.concatenate([base_here] * GROUP, axis=1)
    for j in range(CAPS):
        base[j * GROUP : (j + 1) * GROUP, :] = jnp.broadcast_to(
            base_here[j : j + 1], (GROUP, GROUP * history)
        )
    blocks[...] = (
        lax.broadcasted_iota(jnp.int32, blocks.shape, 0) // history
        == lax.broadcasted_iota(jnp.int32, blocks.shape, 1) // head
    ).astype(F32).astype(BF16)

    table_copy.wait()

    def widen(i, carry):
        at = pl.ds(pl.multiple_of(i * 256, 256), 256)
        for h in range(2):
            table_wide[pl.ds(pl.multiple_of(i * 512, 512) + h, 256, stride=2), :] = table_in[
                at, h * half : (h + 1) * half
            ].astype(F32)
        return carry

    lax.fori_loop(0, table_in.shape[0] // 256, widen, 0)

    own_ids.wait()
    for step in range(n - 1):
        send_ids(step).wait_recv()
    id_copy = pltpu.make_async_copy(ids_vmem, ids_smem, id_sem.at[1])
    id_copy.start()
    id_copy.wait()

    def slot_of(c):
        return pl.multiple_of(lax.rem(c, 2) * 2 * GROUP * history, 2 * GROUP * history)

    def gather(c):
        held = slot_of(c)

        def fetch(u, carry):
            for z in range(n):
                for p in range(span):
                    spot = held + pl.multiple_of(u * 2 * history, 2 * history) + 2 * (z * span + p)
                    rows[pl.ds(spot, 2), :] = table_wide[
                        pl.ds(ids_smem[z, p, c * GROUP + u] * 2, 2), :
                    ]
            return carry

        lax.fori_loop(0, GROUP, fetch, 0)

    ff = w_in.shape[1] - 3 * width
    span_rows = GROUP * history
    lane = lax.broadcasted_iota(jnp.int32, (history, HEADS * history), 1)
    key_spot = lax.rem(lane, history)

    def lengths_of(g):
        length_at = (me * 2 + core) * share + g * GROUP
        return [lens[length_at + u] for u in range(GROUP)]

    def encode(g, first=0, users=GROUP):
        lengths = lengths_of(g)
        span_here = slice(first * history, (first + users) * history)
        count = users * history
        feats_here = recv[pl.ds(g * GROUP + first, users)].reshape(count, width)
        for h in range(2):
            columns = slice(h * half, (h + 1) * half)
            x_ref[span_here, columns] = (
                feats_here[:, columns].astype(F32)
                + rows[pl.ds(slot_of(g) + 2 * first * history + h, count, stride=2), :]
            ).astype(BF16)
        x = x_ref[span_here, :]
        for f in range(0, 3 * width, width):
            qkv[span_here, f : f + width] = dot(x, w_in[:, f : f + width]).astype(BF16)
            yield
        ats = [(u, pl.ds(u * history, history)) for u in range(first, first + users)]
        for u, at in ats:
            keys = jnp.concatenate([qkv[at, width : 2 * width]] * HEADS, axis=0) * blocks[...]
            scores = lax.dot_general(
                qkv[at, :width], keys, NT, preferred_element_type=F32
            ) * (1.0 / head**0.5)
            probs = jnp.where(key_spot < lengths[u], jnp.exp(scores), 0.0)
            top = probs.astype(BF16)
            high[at, :] = top
            low[at, :] = (probs - top.astype(F32)).astype(BF16)
            if u % 2:
                yield
        for f in range(0, ff, 256):
            up = dot(x, w_in[:, 3 * width + f : 3 * width + f + 256])
            mix[span_here, width + f : width + f + 256] = jax.nn.gelu(up).astype(BF16)
            yield
        for u, at in ats:
            values = jnp.concatenate([qkv[at, 2 * width :]] * HEADS, axis=0) * blocks[...]
            weighted[at, :] = dot(high[at, :], values)
            if u % 2:
                yield
        totals = dot(high[span_here, :], blocks[...]) + dot(low[span_here, :], blocks[...])
        mix[span_here, :width] = (weighted[span_here, :] / totals).astype(BF16)
        yield
        made = (dot(x, w_mix[:width, :]) + dot(mix[span_here, :], w_mix[width:, :])).astype(BF16)
        interests[lax.rem(g, 2), span_here, :] = made

    def route(g):
        lengths = lengths_of(g)
        slot = lax.rem(g, 2)
        row = lax.broadcasted_iota(jnp.int32, (GROUP, span_rows), 0)
        col = lax.broadcasted_iota(jnp.int32, (GROUP, span_rows), 1)
        limit = jnp.zeros((GROUP, span_rows), jnp.int32)
        for u in range(GROUP):
            limit = jnp.where(row == u, u * history + lengths[u], limit)
        valid = ((col >= row * history) & (col < limit)).astype(F32)
        logits = [base[j * GROUP : (j + 1) * GROUP, :] for j in range(CAPS)]
        capsules = None
        for sweep in range(ITERS):
            peak = functools.reduce(jnp.maximum, logits)
            powers = [jnp.exp(l - peak) for l in logits]
            scale = valid / functools.reduce(jnp.add, powers)
            weights_here = jnp.concatenate([p * scale for p in powers], axis=0)
            both = dot(split(weights_here), interests[slot])
            yield
            yield
            summed = both[: CAPS * GROUP] + both[CAPS * GROUP :]
            squares = jnp.sum(summed * summed, axis=1, keepdims=True)
            yield
            capsules = summed * (jnp.sqrt(squares) / (1.0 + squares))
            if sweep + 1 < ITERS:
                both = lax.dot_general(
                    split(capsules), interests[slot], NT, preferred_element_type=F32
                )
                yield
                yield
                gain = both[: CAPS * GROUP] + both[CAPS * GROUP :]
                logits = [
                    l + gain[j * GROUP : (j + 1) * GROUP] for j, l in enumerate(logits)
                ]
        mine = jnp.where(core == 0, capsules[:, :half], capsules[:, half:])
        theirs = jnp.where(core == 0, capsules[:, half:], capsules[:, :half])
        first = g * GROUP * CAPS
        for j in range(CAPS):
            here = slice(j * GROUP, (j + 1) * GROUP)
            spot = pl.multiple_of(core * share * CAPS + first, GROUP * CAPS) + j
            out[pl.ds(spot, GROUP, stride=CAPS), :] = mine[here]
            spot = pl.multiple_of(first, GROUP * CAPS) + j
            outbox[pl.ds(spot, GROUP, stride=CAPS), :] = theirs[here]

    size = GROUP * CAPS

    def exchange(c):
        return pltpu.make_async_remote_copy(
            outbox.at[pl.ds(pl.multiple_of(c * size, size), size), :],
            out.at[pl.ds(pl.multiple_of(core * share * CAPS + c * size, size), size), :],
            xsend_sem.at[c],
            xrecv_sem.at[c],
            device_id={"dev": sibling},
            device_id_type=MESH,
        )

    def arrive(p, start, size):
        for step in range(n - 1):
            send_of(p, start, size, step).wait_recv()

    gather(0)
    own_feats.wait()
    for copy in own_copies:
        copy.wait()
    for copy in wcopies:
        copy.wait()

    def advance(c):
        @pl.when(c + lead < chunks)
        def _():
            launch(c + lead, 0)

    gather(1)
    arrive(0, 0, GROUP)
    advance(0)
    interleave(encode(0))

    def consume(c, carry):
        gather(c + 1)
        arrive(c, c * GROUP, GROUP)
        advance(c)
        interleave(route(c - 1), encode(c))

        @pl.when(c > 1)
        def _():
            exchange(c - 2).start()

        return carry

    last = chunks - 1
    lax.fori_loop(1, last - 1, consume, 0)
    exchange(last - 3).start()
    gather(last)
    interleave(route(last - 2))
    arrive(last - 1, (last - 1) * GROUP, GROUP)
    interleave(encode(last - 1))
    exchange(last - 2).start()
    arrive(last, last * GROUP, GROUP)
    interleave(route(last - 1), encode(last))
    exchange(last - 1).start()
    interleave(route(last))
    exchange(last).start()

    def drain(c, carry):
        exchange(c).wait()
        for step in range(n - 1):
            send_of(c, c * GROUP, GROUP, step).wait_send()
        return carry

    for step in range(n - 1):
        send_ids(step).wait_send()
    lax.fori_loop(0, chunks, drain, 0)


def body(
    features, item_ids, item_table, lengths, routing_seed, w_qkv, w_out, w_bilinear, w_up, w_down
):
    n = lax.axis_size("pa")
    cores = lax.axis_size("dev")
    span, width = features.shape[1:]
    owned = lengths.shape[0] // n
    share = owned // cores
    history = n * span
    if (
        cores != 2 or span % 16 or share % 128 or n < 2 or share < 4 * GROUP or history * HEADS != width
        or item_table.shape[0] % 256
    ):
        return plain_body(
            features, item_ids, item_table, lengths, routing_seed,
            w_qkv, w_out, w_bilinear, w_up, w_down,
        )
    chunks = share // GROUP
    rows = GROUP * history
    ff = w_up.shape[1] * cores
    hbm = pl.BlockSpec(memory_space=pltpu.HBM)
    vmem = pl.BlockSpec(memory_space=pltpu.VMEM)
    dma = pltpu.SemaphoreType.DMA
    routed = pl.pallas_call(
        functools.partial(fused, n, share),
        out_shape=jax.ShapeDtypeStruct((owned * CAPS, width // cores), F32),
        in_specs=[hbm] * 10,
        out_specs=vmem,
        scratch_shapes=[
            pltpu.VMEM((n - 1, share, span, width), BF16),
            pltpu.VMEM((share, history, width), BF16),
            pltpu.SMEM(lengths.shape, jnp.int32),
            pltpu.VMEM(routing_seed.shape, jnp.int32),
            pltpu.VMEM((n, span, share), jnp.int32),
            pltpu.SMEM((n, span, share), jnp.int32),
            pltpu.VMEM(item_table.shape, BF16),
            pltpu.VMEM((item_table.shape[0] * 2, width // 2), F32),
            pltpu.VMEM((2 * rows * 2, width // 2), F32),
            pltpu.VMEM((rows, width), BF16),
            pltpu.VMEM((CAPS * GROUP, rows), F32),
            pltpu.VMEM((width, 3 * width + ff), BF16),
            pltpu.VMEM((2 * width + ff, width), BF16),
            pltpu.VMEM((HEADS * history, width), BF16),
            pltpu.VMEM((rows, 3 * width), BF16),
            pltpu.VMEM((rows, width + ff), BF16),
            pltpu.VMEM((rows, width), BF16),
            pltpu.VMEM((rows, width), BF16),
            pltpu.VMEM((rows, width), F32),
            pltpu.VMEM((2, rows, width), BF16),
            pltpu.VMEM((share * CAPS, width // cores), F32),
            dma, dma, dma((n - 1,)), dma((2,)), dma((2,)), dma((n - 1,)), dma((n - 1,)), dma((7,)), dma((7,)), dma((7,)),
            dma((chunks, n - 1)), dma((chunks, n - 1)), dma((chunks,)), dma((chunks,)),
        ],
        compiler_params=pltpu.CompilerParams(
            collective_id=0, has_side_effects=True, vmem_limit_bytes=VMEM_LIMIT
        ),
        name="encode_route",
    )(*(pltpu.with_memory_space_constraint(a, pltpu.HBM) for a in (
        item_ids.T, lengths, features, item_table, routing_seed,
        w_qkv, w_out, w_bilinear, w_up, w_down,
    )))
    return routed.reshape(owned, CAPS, width // cores)


AHEAD = 3
AHEAD_END = 2
VMEM_LIMIT = 50 * 1024 * 1024


def solution(mesh):
    in_specs = (
        P("au", "pa", None),
        P("au", "pa"),
        P(),
        P("au"),
        P(),
        P(None, None, "dev"),
        P("dev", None),
        P(None, "dev"),
        P(None, "dev"),
        P("dev", None),
    )
    out_specs = P(("au", "pa"), None, "dev")
    return jax.shard_map(body, mesh=mesh, in_specs=in_specs, out_specs=out_specs, check_vma=False)
```
